256 devices in a mesh: outer: 16 (over z_lo, x), inner: 16 (over y, z_hi, core).
Axes of the slice: x: 4, y: 4, z: 8 (z_hi: 2, z_lo: 4; z = z_hi * 4 + z_lo), core: 2. Of those that a mesh axis runs over, the one named last changes fastest.
Arguments:
- queries: bfloat16 [8192, 2, 4096], P('outer', None, 'inner'), may hold values from -52 to 52
- keys: bfloat16 [8192, 2, 4096], P('outer', None, 'inner'), may hold values from -6 to 6
- values: bfloat16 [8192, 2, 4096], P('outer', None, 'inner'), may hold values from -6 to 6
Outputs:
- attended: bfloat16 [8192, 2, 4096], P(('outer', 'inner'))
The draws below stay inside these ranges and needn't reach their ends.
All inputs are finite; a program needn't handle non-finite values.
Results may differ from the reference program's by a relative error of at most 0.004.
Values may be sent and summed in bfloat16 or wider, within the bound.
A program may use at most 128 MiB of HBM per device.

```python
import math
import jax
import jax.numpy as jnp
from jax import lax

NETWORKS = 2
HEADS = 32
HEAD_DIM = 128
WIDTH = 4096
SEQ = 8192


def key_field(key):
    base = jax.random.fold_in(key, 11)
    field = jnp.clip(jax.random.normal(base, (SEQ, NETWORKS, WIDTH), jnp.float32), -6.0, 6.0)
    return field


def draw_keys(key, part):
    return key_field(key).astype(jnp.bfloat16)


def draw_queries(key, part):
    base = jax.random.fold_in(key, 12)
    result = 3.0 * jnp.clip(jax.random.normal(base, (SEQ, NETWORKS, WIDTH), jnp.float32), -6.0, 6.0)
    return result.astype(jnp.bfloat16)


def steps_of(rng, shape, shards, low, high):
    factor_of, own = 1.0, jax.random.fold_in(rng, 6)
    for axis_at, shards_of in shards:
        draws = jnp.exp(jax.random.uniform(jax.random.fold_in(own, axis_at), (shards_of,), jnp.float32, low / len(shards), high / len(shards)))
        factor_of = factor_of * jnp.repeat(draws, shape[axis_at] // shards_of).reshape([-1 if axis == axis_at else 1 for axis in range(len(shape))])
    return factor_of


def scatter_about(rng, extent, scale, reach, pieces=(), kind=jnp.bfloat16):
    gain = steps_of(rng, extent, pieces, -0.22, 0.18) if pieces else 1.0
    values = jax.random.normal(rng, extent, jnp.float32) * scale * gain
    return jnp.minimum(jnp.maximum(values, -reach), reach).astype(kind)


def setup_inputs(seed: int = 0) -> dict:
    splits = jax.random.split(jax.random.key(seed), 4)
    queries = draw_queries(jax.random.fold_in(splits[3], 71), 0)
    keys = draw_keys(jax.random.fold_in(splits[3], 71), 0)
    values = scatter_about(splits[2], (SEQ, NETWORKS, WIDTH), 1.0, 6.0, ((0, 16), (2, 16)))
    return dict(queries=queries, keys=keys, values=values)


def attend_rows(query_rows, key_rows, value_rows):
    scores = jnp.dot(query_rows, key_rows.T, preferred_element_type=jnp.float32) * (1.0 / math.sqrt(HEAD_DIM))
    peak_rows = lax.optimization_barrier(jnp.max(scores, axis=1, keepdims=True))
    weights = jnp.exp(scores - peak_rows)
    totals = lax.optimization_barrier(jnp.sum(weights, axis=1, keepdims=True))
    numerator = jnp.dot(weights.astype(jnp.bfloat16), value_rows, preferred_element_type=jnp.float32)
    return numerator / totals

def attend_pair(inputs):
    query_rows, key_rows, value_rows = inputs
    blocks = query_rows.reshape(16, SEQ // 16, HEAD_DIM)
    result = lax.map(lambda block: attend_rows(block, key_rows, value_rows), blocks)
    return result.reshape(SEQ, HEAD_DIM)

def split_heads(array):
    return array.reshape(SEQ, NETWORKS, HEADS, HEAD_DIM).transpose(1, 2, 0, 3).reshape(NETWORKS * HEADS, SEQ, HEAD_DIM)

def reference(queries, keys, values):
    averaged = lax.map(attend_pair, (split_heads(queries), split_heads(keys), split_heads(values)))
    averaged = averaged.reshape(NETWORKS, HEADS, SEQ, HEAD_DIM).transpose(2, 0, 1, 3)
    return averaged.reshape(SEQ, NETWORKS, WIDTH).astype(jnp.bfloat16)
```

```python
import functools
import math

import jax
import jax.numpy as jnp
from jax import lax
from jax.experimental import pallas as pl
from jax.experimental.pallas import tpu as pltpu
from jax.sharding import PartitionSpec as P

HEAD_DIM = 128
XS = 4
ZS = 4
HALVES = 2
FACTOR = math.log2(math.e) / math.sqrt(HEAD_DIM)
MESH = pl.DeviceIdType.MESH


def kernel(
    ni, tok, q_ref, k_ref, v_ref, out_ref,
    qb, kvb, acc, peak, ob, obuf,
    zsend, zrecv, xsend, xrecv, osend, orecv,
):
    half = tok // HALVES
    rows_to = tok // ni
    bq = half
    outer, inner = lax.axis_index("outer"), lax.axis_index("inner")
    x, zl = outer % XS, outer // XS
    core, group = inner % 2, inner // 2
    right, left = (x + 1) % XS, (x + XS - 1) % XS

    def at(x_at, z_at, inner_at):
        return {"outer": z_at * XS + x_at, "inner": inner_at}

    barrier = pltpu.get_barrier_semaphore()

    def hello(index, carry):
        z_at, inner_at = index // ni, index % ni

        @pl.when(jnp.logical_or(z_at != zl, inner_at != inner))
        def _():
            pl.semaphore_signal(barrier, inc=1, device_id=at(x, z_at, inner_at), device_id_type=MESH)

        return carry

    lax.fori_loop(0, ZS * ni, hello, 0)
    for x_at in (left, right):
        pl.semaphore_signal(barrier, inc=1, device_id=at(x_at, zl, inner), device_id_type=MESH)

    acc[...] = jnp.zeros_like(acc)
    peak[...] = jnp.full_like(peak, -1e30)
    keeps = zl // 2 == core
    mine = zl % 2

    @pl.when(keeps)
    def _():
        qb[zl] = q_ref[core, mine]
        for h in range(HALVES):
            kvb[zl, h, x, 0] = k_ref[core, mine, h]
            kvb[zl, h, x, 1] = v_ref[core, mine, h]

    pl.semaphore_wait(barrier, ZS * ni - 1 + 2)

    def z_copy(piece, hh, net):
        z_at = 2 * core + hh
        if piece == 0:
            src, dst = q_ref.at[net, hh], qb.at[zl]
        else:
            h, kv = (piece - 1) // 2, (piece - 1) % 2
            src, dst = (k_ref, v_ref)[kv].at[net, hh, h], kvb.at[zl, h, x, kv]
        return pltpu.make_async_remote_copy(
            src_ref=src, dst_ref=dst,
            send_sem=zsend.at[piece, hh, net], recv_sem=zrecv.at[piece, zl],
            device_id=at(x, z_at, group * 2 + net), device_id_type=MESH,
        )

    def to_all(act):
        for piece in range(1 + 2 * HALVES):
            for hh in range(2):
                for net in range(2):
                    goes = jnp.logical_or(2 * core + hh != zl, net != core)

                    @pl.when(goes)
                    def _(piece=piece, hh=hh, net=net):
                        act(z_copy(piece, hh, net))

    to_all(lambda copy: copy.start())

    def z_of(j):
        flip = zl + 1 - 2 * (zl % 2)
        return ((zl if j % 2 == 0 else flip) + 2 * (j // 2)) % ZS

    def z_wait(piece, z_at):
        if piece == 0:
            ref = qb.at[z_at]
        else:
            h, kv = (piece - 1) // 2, (piece - 1) % 2
            ref = kvb.at[z_at, h, x, kv]
        pltpu.make_async_remote_copy(
            src_ref=ref, dst_ref=ref, send_sem=zsend.at[0, 0, 0], recv_sem=zrecv.at[piece, z_at],
            device_id=at(right, zl, inner), device_id_type=MESH,
        ).wait_recv()

    def z_arrived(piece, j):
        if j == 0:
            @pl.when(jnp.logical_not(keeps))
            def _():
                z_wait(piece, zl)
        else:
            z_wait(piece, z_of(j))

    def x_copy(kind, j, h):
        z_at = z_of(j)
        if kind < 2:
            ref = kvb.at[z_at, h, x]
        elif kind == 2:
            ref = kvb.at[z_at, h, left, 0]
        else:
            ref = kvb.at[z_at, h, right, 1]
        return pltpu.make_async_remote_copy(
            src_ref=ref, dst_ref=ref,
            send_sem=xsend.at[kind, j, h], recv_sem=xrecv.at[kind, j, h],
            device_id=at((right, left)[kind % 2], zl, inner), device_id_type=MESH,
        )

    def x_wait(kind, j, h):
        z_at = z_of(j)
        far = (x + 2) % XS
        ref = (kvb.at[z_at, h, left], kvb.at[z_at, h, right], kvb.at[z_at, h, far, 0], kvb.at[z_at, h, far, 1])[kind]
        pltpu.make_async_remote_copy(
            src_ref=ref, dst_ref=ref, send_sem=xsend.at[kind, j, h], recv_sem=xrecv.at[kind, j, h],
            device_id=at(right, zl, inner), device_id_type=MESH,
        ).wait_recv()

    def stage_a(t):
        j, h = t // HALVES, t % HALVES
        z_arrived(1 + 2 * h, j)
        z_arrived(2 + 2 * h, j)
        x_copy(0, j, h).start()
        x_copy(1, j, h).start()

    def stage_b(t):
        j, h = t // HALVES, t % HALVES
        x_wait(0, j, h)
        x_copy(2, j, h).start()
        x_wait(1, j, h)
        x_copy(3, j, h).start()

    def stage_c(t):
        j, h = t // HALVES, t % HALVES
        x_wait(2, j, h)
        x_wait(3, j, h)

    per = tok // bq

    def attend(t, block):
        j, h = t // HALVES, t % HALVES
        z_at = z_of(j)
        rows = pl.ds(pl.multiple_of(block * bq, bq), bq)
        q = qb[block // per, pl.ds(pl.multiple_of((block % per) * bq, bq), bq)]
        keys = kvb[z_at, h, :, 0].reshape(XS * half, HEAD_DIM)
        values = kvb[z_at, h, :, 1].reshape(XS * half, HEAD_DIM)
        scores = lax.dot_general(q, keys, (((1,), (1,)), ((), ())), preferred_element_type=jnp.float32)
        before = peak[rows]
        now = jnp.maximum(before, jnp.max(scores, axis=1, keepdims=True) * FACTOR)
        peak[rows] = now
        shrink = jnp.exp2(before - now)
        weights = jnp.exp2(scores * FACTOR - jnp.tile(now, (1, XS * half // HEAD_DIM)))
        wide = jnp.concatenate([values, jnp.ones_like(values)], axis=1)
        new = jnp.dot(weights.astype(jnp.bfloat16), wide, preferred_element_type=jnp.float32)
        total = acc[rows] * jnp.tile(shrink, (1, 2)) + new
        return rows, total

    def fold(t):
        def body(block, carry):
            rows, total = attend(t, block)
            acc[rows] = total
            return carry

        lax.fori_loop(0, ZS * per, body, 0)

    steps = ZS * HALVES
    dests = bq // rows_to

    def o_copies(block, act):
        z_at = block // per

        def one(index, carry):
            inner_at = (block % per) * dests + index

            @pl.when(jnp.logical_or(z_at != zl, inner_at != inner))
            def _():
                act(pltpu.make_async_remote_copy(
                    src_ref=ob.at[block * dests + index],
                    dst_ref=obuf.at[core * 2 * ni + group * 4 + zl],
                    send_sem=osend, recv_sem=orecv,
                    device_id=at(x, z_at, inner_at), device_id_type=MESH,
                ))

            return carry

        lax.fori_loop(0, dests, one, 0)

    stage_a(0)
    stage_a(1)
    stage_b(0)
    for j in range(ZS):
        z_arrived(0, j)
    for t in range(steps - 1):
        if t + 2 < steps:
            stage_a(t + 2)
        stage_b(t + 1)
        stage_c(t)
        fold(t)
    stage_c(steps - 1)

    def last(block, carry):
        rows, total = attend(steps - 1, block)
        done = (total[:, :HEAD_DIM] / total[:, HEAD_DIM:]).astype(jnp.bfloat16)
        ob[pl.ds(block * dests, dests)] = done.reshape(dests, rows_to, HEAD_DIM)

        @pl.when(block > 0)
        def _():
            o_copies(block - 1, lambda copy: copy.start())

        return carry

    lax.fori_loop(0, ZS * per, last, 0)
    own = core * 2 * ni + group * 4 + zl
    obuf[own] = ob[zl * ni + inner]
    o_copies(ZS * per - 1, lambda copy: copy.start())

    to_all(lambda copy: copy.wait_send())
    for kind in range(4):
        for j in range(ZS):
            for h in range(HALVES):
                x_copy(kind, j, h).wait_send()
    rest = pltpu.make_async_remote_copy(
        src_ref=obuf.at[pl.ds(0, ZS * ni - 1)], dst_ref=obuf.at[pl.ds(0, ZS * ni - 1)],
        send_sem=osend, recv_sem=orecv, device_id=at(right, zl, inner), device_id_type=MESH,
    )
    rest.wait_send()
    rest.wait_recv()
    out_ref[...] = obuf[...]


def per_device(ni, queries, keys, values):
    tok, nets, cols = queries.shape
    half = tok // HALVES

    def split(a):
        return a.reshape(tok, nets, 2, HEAD_DIM).transpose(1, 2, 0, 3)

    q = split(queries)
    k = split(keys).reshape(nets, 2, HALVES, half, HEAD_DIM)
    v = split(values).reshape(nets, 2, HALVES, half, HEAD_DIM)
    heads = 2 * ni
    rows_to = tok // ni
    vmem = pl.BlockSpec(memory_space=pltpu.VMEM)
    dma = pltpu.SemaphoreType.DMA
    out = pl.pallas_call(
        functools.partial(kernel, ni, tok),
        out_shape=jax.ShapeDtypeStruct((nets * heads, rows_to, HEAD_DIM), jnp.bfloat16),
        in_specs=[vmem] * 3,
        out_specs=vmem,
        scratch_shapes=[
            pltpu.VMEM((ZS, tok, HEAD_DIM), jnp.bfloat16),
            pltpu.VMEM((ZS, HALVES, XS, 2, half, HEAD_DIM), jnp.bfloat16),
            pltpu.VMEM((ZS * tok, 2 * HEAD_DIM), jnp.float32),
            pltpu.VMEM((ZS * tok, HEAD_DIM), jnp.float32),
            pltpu.VMEM((ZS * ni, rows_to, HEAD_DIM), jnp.bfloat16),
            pltpu.VMEM((nets * heads, rows_to, HEAD_DIM), jnp.bfloat16),
            dma((1 + 2 * HALVES, 2, 2)),
            dma((1 + 2 * HALVES, ZS)),
            dma((4, ZS, HALVES)),
            dma((4, ZS, HALVES)),
            dma,
            dma,
        ],
        compiler_params=pltpu.CompilerParams(collective_id=0, has_side_effects=True, vmem_limit_bytes=48 << 20),
        name="attend",
    )(q, k, v)
    return out.reshape(nets, heads, rows_to, HEAD_DIM).transpose(2, 0, 1, 3).reshape(rows_to, nets, heads * HEAD_DIM)


def solution(mesh):
    spec = P("outer", None, "inner")
    return jax.shard_map(
        functools.partial(per_device, mesh.shape["inner"]),
        mesh=mesh,
        in_specs=(spec, spec, spec),
        out_specs=P(("outer", "inner"), None, None),
        check_vma=False,
    )
```

```python
import functools
import math

import jax
import jax.numpy as jnp
from jax import lax
from jax.experimental import pallas as pl
from jax.experimental.pallas import tpu as pltpu
from jax.sharding import PartitionSpec as P

HEAD_DIM = 128
XS = 4
ZS = 4
CUTS = 4
FACTOR = math.log2(math.e) / math.sqrt(HEAD_DIM)
MESH = pl.DeviceIdType.MESH


def kernel(
    ni, tok, q_hbm, k_hbm, v_hbm, out_ref,
    raw, qd, kvd, qb, kvb, acc, peak, ob, obuf,
    score_a, score_b, peak_a, peak_b, shrink_a, shrink_b,
    load, zsend, zrecv, xsend, xrecv, osend, orecv,
):
    piece = tok // CUTS
    rows_to = tok // ni
    keys_at = 2 * XS * piece
    outer, inner = lax.axis_index("outer"), lax.axis_index("inner")
    x, zl = outer % XS, outer // XS
    core, group = inner % 2, inner // 2
    z_hi, y = group % 2, group // 2
    right, left, far = (x + 1) % XS, (x + XS - 1) % XS, (x + 2) % XS

    def at(x_at, z_at, inner_at):
        return {"outer": z_at * XS + x_at, "inner": inner_at}

    loads = [pltpu.make_async_copy(ref, raw.at[i], load.at[i]) for i, ref in enumerate((q_hbm, k_hbm, v_hbm))]
    for copy in loads:
        copy.start()

    barrier = pltpu.get_barrier_semaphore()

    def hello(index, carry):
        z_at, inner_at = index // ni, index % ni

        @pl.when(jnp.logical_or(z_at != zl, inner_at != inner))
        def _():
            pl.semaphore_signal(barrier, inc=1, device_id=at(x, z_at, inner_at), device_id_type=MESH)

        return carry

    lax.fori_loop(0, ZS * ni, hello, 0)
    for x_at in (left, right):
        pl.semaphore_signal(barrier, inc=1, device_id=at(x_at, zl, inner), device_id_type=MESH)

    acc[...] = jnp.zeros_like(acc)
    peak[...] = jnp.full_like(peak, -1e30)

    span = min(128, piece)
    row = lax.broadcasted_iota(jnp.int32, (2 * span, 2 * span), 0)
    col = lax.broadcasted_iota(jnp.int32, (2 * span, 2 * span), 1)
    take = jnp.where(row < span, 2 * row, 2 * (row - span) + 1)
    sort = jnp.where(col == take, 1.0, 0.0).astype(jnp.bfloat16)
    for i in range(3):
        loads[i].wait()
        for s in range(tok // span):
            mixed = raw[i, s * span:(s + 1) * span].reshape(2 * span, 2 * HEAD_DIM)
            parted = jnp.dot(sort, mixed, preferred_element_type=jnp.float32).astype(jnp.bfloat16)
            for net in range(2):
                for hh in range(2):
                    part = parted[net * span:(net + 1) * span, hh * HEAD_DIM:(hh + 1) * HEAD_DIM]
                    if i == 0:
                        qd[net, hh, s * span:(s + 1) * span] = part
                    else:
                        r, off = s * span // piece, s * span % piece
                        kvd[net, hh, r, i - 1, off:off + span] = part

    keeps = zl // 2 == core
    mine, side = zl % 2, zl // 2

    @pl.when(keeps)
    def _():
        qb[zl] = qd[core, mine]
        for r in range(CUTS):
            kvb[zl, r, x] = kvd[core, mine, r]

    pl.semaphore_wait(barrier, ZS * ni - 1 + 2)

    def z_copy(what, hh, net):
        if what == 0:
            src, dst = qd.at[net, hh], qb.at[zl]
        else:
            src, dst = kvd.at[net, hh, what - 1], kvb.at[zl, what - 1, x]
        return pltpu.make_async_remote_copy(
            src_ref=src, dst_ref=dst,
            send_sem=zsend.at[what, hh, net], recv_sem=zrecv.at[what, zl],
            device_id=at(x, 2 * core + hh, group * 2 + net), device_id_type=MESH,
        )

    def to_all(act, order):
        for what in order:
            for hh in range(2):
                for net in range(2):
                    goes = jnp.logical_or(2 * core + hh != zl, net != core)

                    @pl.when(goes)
                    def _(what=what, hh=hh, net=net):
                        act(z_copy(what, hh, net))

    pl.when(keeps)(lambda: to_all(lambda copy: copy.start(), (1, 2, 0, 3, 4)))
    pl.when(jnp.logical_not(keeps))(lambda: to_all(lambda copy: copy.start(), range(1 + CUTS)))

    z_of = (zl, zl + 1 - 2 * mine, (ZS - 1) * (1 - side), 2 - side)

    def wait_for(ref, sem):
        pltpu.make_async_remote_copy(
            src_ref=ref, dst_ref=ref, send_sem=sem, recv_sem=sem,
            device_id=at(right, zl, inner), device_id_type=MESH,
        ).wait_recv()

    def z_arrived(what, j):
        z_at = z_of[j]
        ref = qb.at[z_at] if what == 0 else kvb.at[z_at, what - 1, x]
        if j == 0:
            @pl.when(jnp.logical_not(keeps))
            def _():
                wait_for(ref, zrecv.at[what, z_at])
        else:
            wait_for(ref, zrecv.at[what, z_at])

    def x_copy(kind, j, r):
        block = kvb.at[z_of[j], r]
        ref = (block.at[x], block.at[x], block.at[left, 0], block.at[right, 1])[kind]
        return pltpu.make_async_remote_copy(
            src_ref=ref, dst_ref=ref,
            send_sem=xsend.at[kind, j, r], recv_sem=xrecv.at[kind, j, r],
            device_id=at((right, left)[kind % 2], zl, inner), device_id_type=MESH,
        )

    def x_arrived(kind, j, r):
        block = kvb.at[z_of[j], r]
        ref = (block.at[left], block.at[right], block.at[far, 0], block.at[far, 1])[kind]
        wait_for(ref, xrecv.at[kind, j, r])

    def stage_a(j, r):
        z_arrived(1 + r, j)
        x_copy(0, j, r).start()
        x_copy(1, j, r).start()

    def stage_b(j, r):
        x_arrived(0, j, r)
        x_copy(2, j, r).start()
        x_arrived(1, j, r)
        x_copy(3, j, r).start()

    def stage_c(j, r):
        x_arrived(2, j, r)
        x_arrived(3, j, r)

    buffers = ((score_a, peak_a, shrink_a), (score_b, peak_b, shrink_b))

    def order(b):
        return (zl + b) % ZS

    def rows_of(b):
        return pl.ds(pl.multiple_of(order(b) * tok, tok), tok)

    def scores(z_at, first, b):
        score, top, shrink = buffers[b % 2]
        keys = kvb[z_at, pl.ds(first, 2), :, 0].reshape(keys_at, HEAD_DIM)
        s = lax.dot_general(qb[order(b)], keys, (((1,), (1,)), ((), ())), preferred_element_type=jnp.float32)
        score[...] = s
        before = peak[rows_of(b)]
        now = jnp.maximum(before, jnp.max(s, axis=1, keepdims=True) * FACTOR)
        peak[rows_of(b)] = now
        top[...] = now
        shrink[...] = jnp.exp2(before - now)

    def apply(z_at, first, b):
        score, top, shrink = buffers[b % 2]
        weights = jnp.exp2(score[...] * FACTOR - jnp.tile(top[...], (1, keys_at // HEAD_DIM)))
        values = kvb[z_at, pl.ds(first, 2), :, 1].reshape(keys_at, HEAD_DIM)
        wide = jnp.concatenate([values, jnp.ones_like(values)], axis=1)
        new = jnp.dot(weights.astype(jnp.bfloat16), wide, preferred_element_type=jnp.float32)
        return acc[rows_of(b)] * jnp.tile(shrink[...], (1, 2)) + new

    def fold(z_at, first):
        scores(z_at, first, 0)
        for b in range(ZS):
            if b + 1 < ZS:
                scores(z_at, first, b + 1)
            acc[rows_of(b)] = apply(z_at, first, b)

    def o_send(b):
        z_at = order(b)

        def one(e, carry):
            z_hi_at = jnp.where(e < ni // 2, 1 - z_hi, z_hi) if ni > 2 else z_hi
            y_at = (y + (e % (ni // 2)) // 2) % (ni // 4) if ni > 2 else y
            inner_at = (y_at * 2 + z_hi_at) * 2 + (core + e) % 2

            @pl.when(jnp.logical_or(z_at != zl, inner_at != inner))
            def _():
                pltpu.make_async_remote_copy(
                    src_ref=ob.at[z_at * ni + inner_at],
                    dst_ref=obuf.at[core * 2 * ni + group * 4 + zl],
                    send_sem=osend, recv_sem=orecv,
                    device_id=at(x, z_at, inner_at), device_id_type=MESH,
                ).start()

            return carry

        lax.fori_loop(0, ni, one, 0)

    A, B, C = stage_a, stage_b, stage_c
    for r in range(CUTS):
        A(0, r)
    B(0, 0), B(0, 1), A(1, 0), B(0, 2), A(1, 1), B(0, 3), B(1, 0)
    for j in range(ZS):
        z_arrived(0, j)

    def before0():
        B(1, 1), C(0, 0), C(0, 1)

    def before1():
        A(1, 2), A(2, 0), A(3, 0), C(0, 2), C(0, 3)

    def before2():
        A(1, 3), A(2, 1), B(1, 2), B(2, 0), B(3, 0), C(1, 0), C(1, 1)

    def before3():
        A(2, 2), B(1, 3), B(2, 1), A(2, 3), C(1, 2), C(1, 3)

    def before4():
        B(2, 2), B(2, 3), A(3, 1), C(2, 0), C(2, 1)

    def before5():
        A(3, 2), B(3, 1), A(3, 3), C(2, 2), C(2, 3)

    def before6():
        B(3, 2), B(3, 3), C(3, 0), C(3, 1)

    def chunk(t, carry):
        for step, before in enumerate((before0, before1, before2, before3, before4, before5, before6)):
            pl.when(t == step)(before)
        near, across = jnp.where(t < 2, z_of[0], z_of[1]), jnp.where(t < 6, z_of[2], z_of[3])
        fold(jnp.where(t < 4, near, across), t % 2 * 2)
        return carry

    lax.fori_loop(0, 7, chunk, 0)
    C(3, 2), C(3, 3)

    last = (z_of[3], 2)
    scores(*last, 0)
    for b in range(ZS):
        if b + 1 < ZS:
            scores(*last, b + 1)
        total = apply(*last, b)
        done = (total[:, :HEAD_DIM] / total[:, HEAD_DIM:]).astype(jnp.bfloat16)
        ob[pl.ds(order(b) * ni, ni)] = done.reshape(ni, rows_to, HEAD_DIM)
        o_send(b)
    own = core * 2 * ni + group * 4 + zl
    obuf[own] = ob[zl * ni + inner]

    to_all(lambda copy: copy.wait_send(), range(1 + CUTS))
    for kind in range(4):
        for j in range(ZS):
            for r in range(CUTS):
                x_copy(kind, j, r).wait_send()
    rest = pltpu.make_async_remote_copy(
        src_ref=obuf.at[pl.ds(0, ZS * ni - 1)], dst_ref=obuf.at[pl.ds(0, ZS * ni - 1)],
        send_sem=osend, recv_sem=orecv, device_id=at(right, zl, inner), device_id_type=MESH,
    )
    rest.wait_send()
    rest.wait_recv()
    out_ref[...] = obuf[...]


def per_device(ni, queries, keys, values):
    tok, nets, cols = queries.shape
    heads = 2 * ni
    rows_to = tok // ni
    piece = tok // CUTS
    hbm = pl.BlockSpec(memory_space=pltpu.HBM)
    dma = pltpu.SemaphoreType.DMA
    bf16, f32 = jnp.bfloat16, jnp.float32
    out = pl.pallas_call(
        functools.partial(kernel, ni, tok),
        out_shape=jax.ShapeDtypeStruct((nets * heads, rows_to, HEAD_DIM), bf16),
        in_specs=[hbm] * 3,
        out_specs=pl.BlockSpec(memory_space=pltpu.VMEM),
        scratch_shapes=[
            pltpu.VMEM((3, tok, nets, cols), bf16),
            pltpu.VMEM((nets, 2, tok, HEAD_DIM), bf16),
            pltpu.VMEM((nets, 2, CUTS, 2, piece, HEAD_DIM), bf16),
            pltpu.VMEM((ZS, tok, HEAD_DIM), bf16),
            pltpu.VMEM((ZS, CUTS, XS, 2, piece, HEAD_DIM), bf16),
            pltpu.VMEM((ZS * tok, 2 * HEAD_DIM), f32),
            pltpu.VMEM((ZS * tok, HEAD_DIM), f32),
            pltpu.VMEM((ZS * ni, rows_to, HEAD_DIM), bf16),
            pltpu.VMEM((nets * heads, rows_to, HEAD_DIM), bf16),
            pltpu.VMEM((tok, 2 * XS * piece), f32),
            pltpu.VMEM((tok, 2 * XS * piece), f32),
            pltpu.VMEM((tok, HEAD_DIM), f32),
            pltpu.VMEM((tok, HEAD_DIM), f32),
            pltpu.VMEM((tok, HEAD_DIM), f32),
            pltpu.VMEM((tok, HEAD_DIM), f32),
            dma((3,)),
            dma((1 + CUTS, 2, 2)),
            dma((1 + CUTS, ZS)),
            dma((4, ZS, CUTS)),
            dma((4, ZS, CUTS)),
            dma,
            dma,
        ],
        compiler_params=pltpu.CompilerParams(collective_id=0, has_side_effects=True, vmem_limit_bytes=56 << 20),
        name="attend",
    )(queries, keys, values)
    return out.reshape(nets, heads, rows_to, HEAD_DIM).transpose(2, 0, 1, 3).reshape(rows_to, nets, heads * HEAD_DIM)


def solution(mesh):
    spec = P("outer", None, "inner")
    return jax.shard_map(
        functools.partial(per_device, mesh.shape["inner"]),
        mesh=mesh,
        in_specs=(spec, spec, spec),
        out_specs=P(("outer", "inner"), None, None),
        check_vma=False,
    )
```

```python
import functools
import math

import jax
import jax.numpy as jnp
from jax import lax
from jax.experimental import pallas as pl
from jax.experimental.pallas import tpu as pltpu
from jax.sharding import PartitionSpec as P

HEAD_DIM = 128
XS = 4
ZS = 4
CUTS = 4
FACTOR = math.log2(math.e) / math.sqrt(HEAD_DIM)
MESH = pl.DeviceIdType.MESH


def kernel(
    ni, tok, q_hbm, k_hbm, v_hbm, out_ref,
    raw, qd, kvd, qb, kvb, acc, peak, ob, obuf,
    score_a, score_b, peak_a, peak_b, shrink_a, shrink_b,
    load, zsend, zrecv, xsend, xrecv, osend, orecv,
):
    piece = tok // CUTS
    rows_to = tok // ni
    outer, inner = lax.axis_index("outer"), lax.axis_index("inner")
    x, zl = outer % XS, outer // XS
    core, group = inner % 2, inner // 2
    z_hi, y = group % 2, group // 2
    right, left, far = (x + 1) % XS, (x + XS - 1) % XS, (x + 2) % XS

    def at(x_at, z_at, inner_at):
        return {"outer": z_at * XS + x_at, "inner": inner_at}

    loads = [pltpu.make_async_copy(ref, raw.at[i], load.at[i]) for i, ref in enumerate((q_hbm, k_hbm, v_hbm))]
    for copy in loads:
        copy.start()

    barrier = pltpu.get_barrier_semaphore()

    def hello(index, carry):
        z_at, inner_at = index // ni, index % ni

        @pl.when(jnp.logical_or(z_at != zl, inner_at != inner))
        def _():
            pl.semaphore_signal(barrier, inc=1, device_id=at(x, z_at, inner_at), device_id_type=MESH)

        return carry

    lax.fori_loop(0, ZS * ni, hello, 0)
    for x_at in (left, right):
        pl.semaphore_signal(barrier, inc=1, device_id=at(x_at, zl, inner), device_id_type=MESH)

    acc[...] = jnp.zeros_like(acc)
    peak[...] = jnp.full_like(peak, -1e30)

    span = min(128, piece)
    row = lax.broadcasted_iota(jnp.int32, (2 * span, 2 * span), 0)
    col = lax.broadcasted_iota(jnp.int32, (2 * span, 2 * span), 1)
    take = jnp.where(row < span, 2 * row, 2 * (row - span) + 1)
    sort = jnp.where(col == take, 1.0, 0.0).astype(jnp.bfloat16)
    for i in range(3):
        loads[i].wait()
        for s in range(tok // span):
            mixed = raw[i, s * span:(s + 1) * span].reshape(2 * span, 2 * HEAD_DIM)
            parted = jnp.dot(sort, mixed, preferred_element_type=jnp.float32).astype(jnp.bfloat16)
            for net in range(2):
                for hh in range(2):
                    part = parted[net * span:(net + 1) * span, hh * HEAD_DIM:(hh + 1) * HEAD_DIM]
                    if i == 0:
                        qd[net, hh, s * span:(s + 1) * span] = part
                    else:
                        r, off = s * span // piece, s * span % piece
                        kvd[net, hh, r, i - 1, off:off + span] = part

    keeps = zl // 2 == core
    mine, side = zl % 2, zl // 2

    @pl.when(keeps)
    def _():
        qb[zl] = qd[core, mine]
        for r in range(CUTS):
            kvb[zl, r, x] = kvd[core, mine, r]

    pl.semaphore_wait(barrier, ZS * ni - 1 + 2)

    def z_copy(what, hh, net):
        if what == 0:
            src, dst = qd.at[net, hh], qb.at[zl]
        else:
            src, dst = kvd.at[net, hh, what - 1], kvb.at[zl, what - 1, x]
        return pltpu.make_async_remote_copy(
            src_ref=src, dst_ref=dst,
            send_sem=zsend.at[what, hh, net], recv_sem=zrecv.at[what, zl],
            device_id=at(x, 2 * core + hh, group * 2 + net), device_id_type=MESH,
        )

    def to_all(act, order):
        for what in order:
            for hh in range(2):
                for net in range(2):
                    goes = jnp.logical_or(2 * core + hh != zl, net != core)

                    @pl.when(goes)
                    def _(what=what, hh=hh, net=net):
                        act(z_copy(what, hh, net))

    across = jnp.logical_not(keeps)
    at_end = jnp.logical_or(zl == 0, zl == ZS - 1)

    def start(cond, order):
        pl.when(cond)(lambda: to_all(lambda copy: copy.start(), order))

    start(keeps, (1, 2, 0, 3, 4))
    start(jnp.logical_and(across, at_end), (0, 1, 2, 3, 4))
    start(jnp.logical_and(across, jnp.logical_not(at_end)), (1, 2, 3, 4, 0))

    z_of = (zl, zl + 1 - 2 * mine, (ZS - 1) * (1 - side), 2 - side)

    def wait_for(ref, sem):
        pltpu.make_async_remote_copy(
            src_ref=ref, dst_ref=ref, send_sem=sem, recv_sem=sem,
            device_id=at(right, zl, inner), device_id_type=MESH,
        ).wait_recv()

    def z_arrived(what, j):
        z_at = z_of[j]
        ref = qb.at[z_at] if what == 0 else kvb.at[z_at, what - 1, x]
        if j == 0:
            @pl.when(jnp.logical_not(keeps))
            def _():
                wait_for(ref, zrecv.at[what, z_at])
        else:
            wait_for(ref, zrecv.at[what, z_at])

    def x_copy(kind, j, r):
        block = kvb.at[z_of[j], r]
        ref = (block.at[x], block.at[x], block.at[left, 0], block.at[right, 1])[kind]
        return pltpu.make_async_remote_copy(
            src_ref=ref, dst_ref=ref,
            send_sem=xsend.at[kind, j, r], recv_sem=xrecv.at[kind, j, r],
            device_id=at((right, left)[kind % 2], zl, inner), device_id_type=MESH,
        )

    def x_arrived(kind, j, r):
        block = kvb.at[z_of[j], r]
        ref = (block.at[left], block.at[right], block.at[far, 0], block.at[far, 1])[kind]
        wait_for(ref, xrecv.at[kind, j, r])

    def stage_a(j, r):
        z_arrived(1 + r, j)
        x_copy(0, j, r).start()
        x_copy(1, j, r).start()

    def stage_b(j, r):
        x_arrived(0, j, r)
        x_copy(2, j, r).start()
        x_arrived(1, j, r)
        x_copy(3, j, r).start()

    def stage_c(j, r):
        x_arrived(2, j, r)
        x_arrived(3, j, r)

    width = 2 * XS * piece
    buffers = ((score_a, peak_a, shrink_a), (score_b, peak_b, shrink_b))

    def order(b):
        return z_of[b]

    def rows_of(b):
        return pl.ds(pl.multiple_of(order(b) * tok, tok), tok)

    def scores(z_at, first, b, into):
        score, top, shrink = buffers[into % 2]
        keys = kvb[z_at, pl.ds(first, 2), :, 0].reshape(width, HEAD_DIM)
        s = lax.dot_general(qb[order(b)], keys, (((1,), (1,)), ((), ())), preferred_element_type=jnp.float32)
        score[...] = s
        before = peak[rows_of(b)]
        now = jnp.maximum(before, jnp.max(s, axis=1, keepdims=True) * FACTOR)
        peak[rows_of(b)] = now
        top[...] = now
        shrink[...] = jnp.exp2(before - now)

    def apply(z_at, first, b, into):
        score, top, shrink = buffers[into % 2]
        weights = jnp.exp2(score[...] * FACTOR - jnp.tile(top[...], (1, width // HEAD_DIM)))
        values = kvb[z_at, pl.ds(first, 2), :, 1].reshape(width, HEAD_DIM)
        wide = jnp.concatenate([values, jnp.ones_like(values)], axis=1)
        new = jnp.dot(weights.astype(jnp.bfloat16), wide, preferred_element_type=jnp.float32)
        return acc[rows_of(b)] * jnp.tile(shrink[...], (1, 2)) + new

    def fold(keys, between):
        scores(*keys, 0, 0)
        for b in range(ZS - 1):
            between(1 + b)
            if b + 2 < ZS:
                scores(*keys, b + 1, b + 1)
            acc[rows_of(b)] = apply(*keys, b, b)

    slot = core * 2 * ni + group * 4 + zl

    def o_send(b):
        z_at = order(b)
        for e in range(ni):
            z_hi_at = (1 - z_hi if e < ni // 2 else z_hi) if ni > 2 else z_hi
            y_at = (y + 1 + (e % (ni // 2)) // 2) % (ni // 4) if ni > 2 else y
            inner_at = (y_at * 2 + z_hi_at) * 2 + (core + 1 + e) % 2
            if b == 0 and e == ni - 1:
                continue
            pltpu.make_async_remote_copy(
                src_ref=ob.at[z_at * ni + inner_at], dst_ref=obuf.at[slot], send_sem=osend, recv_sem=orecv,
                device_id=at(x, z_at, inner_at), device_id_type=MESH,
            ).start()

    def finish(b, total):
        done = (total[:, :HEAD_DIM] / total[:, HEAD_DIM:]).astype(jnp.bfloat16)
        ob[pl.ds(order(b) * ni, ni)] = done.reshape(ni, rows_to, HEAD_DIM)
        o_send(b)

    A, B, C = stage_a, stage_b, stage_c
    for r in range(CUTS):
        A(0, r)
    B(0, 0), A(1, 0), B(0, 1), A(3, 0), B(0, 2), A(1, 1), B(0, 3), B(1, 0)
    for j in range(ZS - 1):
        z_arrived(0, j)

    chunks = ((0, 0), (0, 2), (1, 0), (3, 0), (1, 2), (2, 0), (2, 2), (3, 2))
    plan = (
        ((C, 0, 0), (C, 0, 1)), ((B, 3, 0),), ((A, 3, 1),), ((B, 1, 1),),
        ((C, 0, 2), (C, 0, 3)), (), ((A, 1, 2),), ((B, 3, 1),),
        ((C, 1, 0), (C, 1, 1)), ((A, 3, 2), (A, 2, 0)), ((A, 1, 3),), ((B, 1, 2),),
        ((C, 3, 0), (C, 3, 1)), ((A, 2, 1),), ((B, 3, 2), (B, 2, 0)), ((B, 1, 3),),
        ((A, 2, 2), (B, 2, 1), (C, 1, 2), (C, 1, 3)), ((A, 2, 3),), ((B, 2, 2),), (),
        ((C, 2, 0), (C, 2, 1)), ((A, 3, 3),), (), ((B, 2, 3),),
        ((B, 3, 3), (C, 2, 2), (C, 2, 3)), (), (), (),
    )

    for t in range(7):
        def moves(slot_at, t=t):
            for act, j, r in plan[t * ZS + slot_at]:
                act(j, r)

        z_at, first = z_of[chunks[t][0]], chunks[t][1]
        moves(0)
        fold((z_at, first), moves)

    late = ZS - 1

    def of(step):
        return z_of[chunks[step][0]], chunks[step][1]

    C(3, 2), C(3, 3)
    scores(*of(7), 0, 0)
    for b in range(ZS - 1):
        if b + 2 < ZS:
            scores(*of(7), b + 1, b + 1)
        finish(b, apply(*of(7), b, b))
    z_arrived(0, 3)
    scores(*of(0), late, 0)
    for step in range(7):
        scores(*of(step + 1), late, step + 1)
        acc[rows_of(late)] = apply(*of(step), late, step)
    finish(late, apply(*of(7), late, 7))
    obuf[slot] = ob[zl * ni + inner]

    to_all(lambda copy: copy.wait_send(), range(1 + CUTS))
    for kind in range(4):
        for j in range(ZS):
            for r in range(CUTS):
                x_copy(kind, j, r).wait_send()
    rest = pltpu.make_async_remote_copy(
        src_ref=obuf.at[pl.ds(0, ZS * ni - 1)], dst_ref=obuf.at[pl.ds(0, ZS * ni - 1)],
        send_sem=osend, recv_sem=orecv, device_id=at(right, zl, inner), device_id_type=MESH,
    )
    rest.wait_send()
    rest.wait_recv()
    out_ref[...] = obuf[...]


def per_device(ni, queries, keys, values):
    tok, nets, cols = queries.shape
    heads = 2 * ni
    rows_to = tok // ni
    piece = tok // CUTS
    hbm = pl.BlockSpec(memory_space=pltpu.HBM)
    dma = pltpu.SemaphoreType.DMA
    bf16, f32 = jnp.bfloat16, jnp.float32
    out = pl.pallas_call(
        functools.partial(kernel, ni, tok),
        out_shape=jax.ShapeDtypeStruct((nets * heads, rows_to, HEAD_DIM), bf16),
        in_specs=[hbm] * 3,
        out_specs=pl.BlockSpec(memory_space=pltpu.VMEM),
        scratch_shapes=[
            pltpu.VMEM((3, tok, nets, cols), bf16),
            pltpu.VMEM((nets, 2, tok, HEAD_DIM), bf16),
            pltpu.VMEM((nets, 2, CUTS, 2, piece, HEAD_DIM), bf16),
            pltpu.VMEM((ZS, tok, HEAD_DIM), bf16),
            pltpu.VMEM((ZS, CUTS, XS, 2, piece, HEAD_DIM), bf16),
            pltpu.VMEM((ZS * tok, 2 * HEAD_DIM), f32),
            pltpu.VMEM((ZS * tok, HEAD_DIM), f32),
            pltpu.VMEM((ZS * ni, rows_to, HEAD_DIM), bf16),
            pltpu.VMEM((nets * heads, rows_to, HEAD_DIM), bf16),
            pltpu.VMEM((tok, 2 * XS * piece), f32),
            pltpu.VMEM((tok, 2 * XS * piece), f32),
            pltpu.VMEM((tok, HEAD_DIM), f32),
            pltpu.VMEM((tok, HEAD_DIM), f32),
            pltpu.VMEM((tok, HEAD_DIM), f32),
            pltpu.VMEM((tok, HEAD_DIM), f32),
            dma((3,)),
            dma((1 + CUTS, 2, 2)),
            dma((1 + CUTS, ZS)),
            dma((4, ZS, CUTS)),
            dma((4, ZS, CUTS)),
            dma,
            dma,
        ],
        compiler_params=pltpu.CompilerParams(collective_id=0, has_side_effects=True, vmem_limit_bytes=56 << 20),
        name="attend",
    )(queries, keys, values)
    return out.reshape(nets, heads, rows_to, HEAD_DIM).transpose(2, 0, 1, 3).reshape(rows_to, nets, heads * HEAD_DIM)


def solution(mesh):
    spec = P("outer", None, "inner")
    return jax.shard_map(
        functools.partial(per_device, mesh.shape["inner"]),
        mesh=mesh,
        in_specs=(spec, spec, spec),
        out_specs=P(("outer", "inner"), None, None),
        check_vma=False,
    )
```

```python
import functools
import math

import jax
import jax.numpy as jnp
from jax import lax
from jax.experimental import pallas as pl
from jax.experimental.pallas import tpu as pltpu
from jax.sharding import PartitionSpec as P

HEAD_DIM = 128
XS = 4
ZS = 4
CUTS = 4
FACTOR = math.log2(math.e) / math.sqrt(HEAD_DIM)
MESH = pl.DeviceIdType.MESH


def kernel(
    ni, tok, q_hbm, k_hbm, v_hbm, out_ref,
    raw, qd, kvd, qb, kvb, acc, peak, ob, obuf,
    score_a, score_b, peak_a, peak_b, shrink_a, shrink_b,
    load, zsend, zrecv, xsend, xrecv, osend, orecv,
):
    piece = tok // CUTS
    rows_to = tok // ni
    outer, inner = lax.axis_index("outer"), lax.axis_index("inner")
    x, zl = outer % XS, outer // XS
    core, group = inner % 2, inner // 2
    z_hi, y = group % 2, group // 2
    right, left, far = (x + 1) % XS, (x + XS - 1) % XS, (x + 2) % XS

    def at(x_at, z_at, inner_at):
        return {"outer": z_at * XS + x_at, "inner": inner_at}

    loads = [pltpu.make_async_copy(ref, raw.at[i], load.at[i]) for i, ref in enumerate((q_hbm, k_hbm, v_hbm))]
    for copy in loads:
        copy.start()

    barrier = pltpu.get_barrier_semaphore()

    def hello(index, carry):
        z_at, inner_at = index // ni, index % ni

        @pl.when(jnp.logical_or(z_at != zl, inner_at != inner))
        def _():
            pl.semaphore_signal(barrier, inc=1, device_id=at(x, z_at, inner_at), device_id_type=MESH)

        return carry

    lax.fori_loop(0, ZS * ni, hello, 0)
    for x_at in (left, right):
        pl.semaphore_signal(barrier, inc=1, device_id=at(x_at, zl, inner), device_id_type=MESH)

    acc[...] = jnp.zeros_like(acc)
    peak[...] = jnp.full_like(peak, -1e30)

    span = min(128, piece)
    row = lax.broadcasted_iota(jnp.int32, (2 * span, 2 * span), 0)
    col = lax.broadcasted_iota(jnp.int32, (2 * span, 2 * span), 1)
    take = jnp.where(row < span, 2 * row, 2 * (row - span) + 1)
    sort = jnp.where(col == take, 1.0, 0.0).astype(jnp.bfloat16)
    for i in range(3):
        loads[i].wait()
        for s in range(tok // span):
            mixed = raw[i, s * span:(s + 1) * span].reshape(2 * span, 2 * HEAD_DIM)
            parted = jnp.dot(sort, mixed, preferred_element_type=jnp.float32).astype(jnp.bfloat16)
            for net in range(2):
                for hh in range(2):
                    part = parted[net * span:(net + 1) * span, hh * HEAD_DIM:(hh + 1) * HEAD_DIM]
                    if i == 0:
                        qd[net, hh, s * span:(s + 1) * span] = part
                    else:
                        r, off = s * span // piece, s * span % piece
                        kvd[net, hh, r, i - 1, off:off + span] = part

    keeps = zl // 2 == core
    mine, side = zl % 2, zl // 2

    @pl.when(keeps)
    def _():
        qb[zl] = qd[core, mine]
        for r in range(CUTS):
            kvb[zl, r, x] = kvd[core, mine, r]

    pl.semaphore_wait(barrier, ZS * ni - 1 + 2)

    def z_copy(what, hh, net):
        if what == 0:
            src, dst = qd.at[net, hh], qb.at[zl]
        else:
            src, dst = kvd.at[net, hh, what - 1], kvb.at[zl, what - 1, x]
        return pltpu.make_async_remote_copy(
            src_ref=src, dst_ref=dst,
            send_sem=zsend.at[what, hh, net], recv_sem=zrecv.at[what, zl],
            device_id=at(x, 2 * core + hh, group * 2 + net), device_id_type=MESH,
        )

    def to_all(act, order):
        for what in order:
            for hh in range(2):
                for net in range(2):
                    goes = jnp.logical_or(2 * core + hh != zl, net != core)

                    @pl.when(goes)
                    def _(what=what, hh=hh, net=net):
                        act(z_copy(what, hh, net))

    across = jnp.logical_not(keeps)
    at_end = jnp.logical_or(zl == 0, zl == ZS - 1)

    def start(cond, order):
        pl.when(cond)(lambda: to_all(lambda copy: copy.start(), order))

    start(keeps, (1, 2, 0, 3, 4))
    start(jnp.logical_and(across, at_end), (0, 1, 2, 3, 4))
    start(jnp.logical_and(across, jnp.logical_not(at_end)), (1, 2, 3, 4, 0))

    z_of = (zl, zl + 1 - 2 * mine, (ZS - 1) * (1 - side), 2 - side)

    def wait_for(ref, sem):
        pltpu.make_async_remote_copy(
            src_ref=ref, dst_ref=ref, send_sem=sem, recv_sem=sem,
            device_id=at(right, zl, inner), device_id_type=MESH,
        ).wait_recv()

    def z_arrived(what, j):
        z_at = z_of[j]
        ref = qb.at[z_at] if what == 0 else kvb.at[z_at, what - 1, x]
        if j == 0:
            @pl.when(jnp.logical_not(keeps))
            def _():
                wait_for(ref, zrecv.at[what, z_at])
        else:
            wait_for(ref, zrecv.at[what, z_at])

    def x_copy(kind, j, r):
        block = kvb.at[z_of[j], r]
        ref = (block.at[x], block.at[x], block.at[left, 0], block.at[right, 1])[kind]
        return pltpu.make_async_remote_copy(
            src_ref=ref, dst_ref=ref,
            send_sem=xsend.at[kind, j, r], recv_sem=xrecv.at[kind, j, r],
            device_id=at((right, left)[kind % 2], zl, inner), device_id_type=MESH,
        )

    def x_arrived(kind, j, r):
        block = kvb.at[z_of[j], r]
        ref = (block.at[left], block.at[right], block.at[far, 0], block.at[far, 1])[kind]
        wait_for(ref, xrecv.at[kind, j, r])

    def stage_a(j, r):
        z_arrived(1 + r, j)
        x_copy(0, j, r).start()
        x_copy(1, j, r).start()

    def stage_b(j, r):
        x_arrived(0, j, r)
        x_copy(2, j, r).start()
        x_arrived(1, j, r)
        x_copy(3, j, r).start()

    def stage_c(j, r):
        x_arrived(2, j, r)
        x_arrived(3, j, r)

    width = 2 * XS * piece
    buffers = ((score_a, peak_a, shrink_a), (score_b, peak_b, shrink_b))

    def order(b):
        return z_of[b]

    def rows_of(b):
        return pl.ds(pl.multiple_of(order(b) * tok, tok), tok)

    def scores(z_at, first, b, into):
        score, top, shrink = buffers[into % 2]
        keys = kvb[z_at, pl.ds(first, 2), :, 0].reshape(width, HEAD_DIM)
        s = lax.dot_general(qb[order(b)], keys, (((1,), (1,)), ((), ())), preferred_element_type=jnp.float32)
        score[...] = s
        before = peak[rows_of(b)]
        now = jnp.maximum(before, jnp.max(s, axis=1, keepdims=True) * FACTOR)
        peak[rows_of(b)] = now
        top[...] = now
        shrink[...] = jnp.exp2(before - now)

    def apply(z_at, first, b, into):
        score, top, shrink = buffers[into % 2]
        weights = jnp.exp2(score[...] * FACTOR - jnp.tile(top[...], (1, width // HEAD_DIM)))
        values = kvb[z_at, pl.ds(first, 2), :, 1].reshape(width, HEAD_DIM)
        wide = jnp.concatenate([values, jnp.ones_like(values)], axis=1)
        new = jnp.dot(weights.astype(jnp.bfloat16), wide, preferred_element_type=jnp.float32)
        return acc[rows_of(b)] * jnp.tile(shrink[...], (1, 2)) + new

    def fold(*keys):
        scores(*keys, 0, 0)
        for b in range(ZS - 1):
            if b + 2 < ZS:
                scores(*keys, b + 1, b + 1)
            acc[rows_of(b)] = apply(*keys, b, b)

    slot = core * 2 * ni + group * 4 + zl

    def o_send(b):
        z_at = order(b)
        for e in range(ni):
            z_hi_at = (1 - z_hi if e < ni // 2 else z_hi) if ni > 2 else z_hi
            y_at = (y + 1 + (e % (ni // 2)) // 2) % (ni // 4) if ni > 2 else y
            inner_at = (y_at * 2 + z_hi_at) * 2 + (core + 1 + e) % 2
            if b == 0 and e == ni - 1:
                continue
            pltpu.make_async_remote_copy(
                src_ref=ob.at[z_at * ni + inner_at], dst_ref=obuf.at[slot], send_sem=osend, recv_sem=orecv,
                device_id=at(x, z_at, inner_at), device_id_type=MESH,
            ).start()

    def finish(b, total):
        done = (total[:, :HEAD_DIM] / total[:, HEAD_DIM:]).astype(jnp.bfloat16)
        ob[pl.ds(order(b) * ni, ni)] = done.reshape(ni, rows_to, HEAD_DIM)
        o_send(b)

    A, B, C = stage_a, stage_b, stage_c
    for r in range(CUTS):
        A(0, r)
    B(0, 0), A(1, 0), B(0, 1), A(3, 0), B(0, 2), A(1, 1), B(0, 3), B(1, 0)
    for j in range(ZS - 1):
        z_arrived(0, j)

    chunks = ((0, 0), (0, 2), (1, 0), (3, 0), (1, 2), (2, 0), (2, 2), (3, 2))
    def of(step):
        return z_of[chunks[step][0]], chunks[step][1]

    plan = (
        ((C, 0, 0), (C, 0, 1)),
        ((B, 3, 0), (A, 3, 1), (B, 1, 1), (C, 0, 2), (C, 0, 3)),
        ((A, 1, 2), (B, 3, 1), (A, 2, 0), (A, 3, 2), (C, 1, 0), (C, 1, 1)),
        ((A, 1, 3), (A, 2, 1), (B, 1, 2), (B, 3, 2), (B, 2, 0), (A, 2, 2), (C, 3, 0), (C, 3, 1)),
        ((B, 1, 3), (A, 2, 3), (B, 2, 1), (C, 1, 2), (A, 3, 3), (C, 1, 3)),
        ((B, 2, 2), (C, 2, 0), (C, 2, 1), (B, 2, 3)),
        ((B, 3, 3), (C, 2, 2), (C, 2, 3)),
    )
    for step in range(7):
        for act, j, r in plan[step]:
            act(j, r)
        fold(*of(step))

    late = ZS - 1


    def catch_up(begin, end):
        scores(*of(begin), late, begin)
        for step in range(begin, end):
            if step + 1 < end:
                scores(*of(step + 1), late, step + 1)
            total = apply(*of(step), late, step)
            if step == 7:
                finish(late, total)
            else:
                acc[rows_of(late)] = total

    C(3, 2), C(3, 3)
    scores(*of(7), 0, 0)
    for b in range(ZS - 1):
        if b + 2 < ZS:
            scores(*of(7), b + 1, b + 1)
        finish(b, apply(*of(7), b, b))
    z_arrived(0, 3)
    catch_up(0, 8)
    obuf[slot] = ob[zl * ni + inner]

    to_all(lambda copy: copy.wait_send(), range(1 + CUTS))
    for kind in range(4):
        for j in range(ZS):
            for r in range(CUTS):
                x_copy(kind, j, r).wait_send()
    rest = pltpu.make_async_remote_copy(
        src_ref=obuf.at[pl.ds(0, ZS * ni - 1)], dst_ref=obuf.at[pl.ds(0, ZS * ni - 1)],
        send_sem=osend, recv_sem=orecv, device_id=at(right, zl, inner), device_id_type=MESH,
    )
    rest.wait_send()
    rest.wait_recv()
    out_ref[...] = obuf[...]


def per_device(ni, queries, keys, values):
    tok, nets, cols = queries.shape
    heads = 2 * ni
    rows_to = tok // ni
    piece = tok // CUTS
    hbm = pl.BlockSpec(memory_space=pltpu.HBM)
    dma = pltpu.SemaphoreType.DMA
    bf16, f32 = jnp.bfloat16, jnp.float32
    out = pl.pallas_call(
        functools.partial(kernel, ni, tok),
        out_shape=jax.ShapeDtypeStruct((nets * heads, rows_to, HEAD_DIM), bf16),
        in_specs=[hbm] * 3,
        out_specs=pl.BlockSpec(memory_space=pltpu.VMEM),
        scratch_shapes=[
            pltpu.VMEM((3, tok, nets, cols), bf16),
            pltpu.VMEM((nets, 2, tok, HEAD_DIM), bf16),
            pltpu.VMEM((nets, 2, CUTS, 2, piece, HEAD_DIM), bf16),
            pltpu.VMEM((ZS, tok, HEAD_DIM), bf16),
            pltpu.VMEM((ZS, CUTS, XS, 2, piece, HEAD_DIM), bf16),
            pltpu.VMEM((ZS * tok, 2 * HEAD_DIM), f32),
            pltpu.VMEM((ZS * tok, HEAD_DIM), f32),
            pltpu.VMEM((ZS * ni, rows_to, HEAD_DIM), bf16),
            pltpu.VMEM((nets * heads, rows_to, HEAD_DIM), bf16),
            pltpu.VMEM((tok, 2 * XS * piece), f32),
            pltpu.VMEM((tok, 2 * XS * piece), f32),
            pltpu.VMEM((tok, HEAD_DIM), f32),
            pltpu.VMEM((tok, HEAD_DIM), f32),
            pltpu.VMEM((tok, HEAD_DIM), f32),
            pltpu.VMEM((tok, HEAD_DIM), f32),
            dma((3,)),
            dma((1 + CUTS, 2, 2)),
            dma((1 + CUTS, ZS)),
            dma((4, ZS, CUTS)),
            dma((4, ZS, CUTS)),
            dma,
            dma,
        ],
        compiler_params=pltpu.CompilerParams(collective_id=0, has_side_effects=True, vmem_limit_bytes=56 << 20),
        name="attend",
    )(queries, keys, values)
    return out.reshape(nets, heads, rows_to, HEAD_DIM).transpose(2, 0, 1, 3).reshape(rows_to, nets, heads * HEAD_DIM)


def solution(mesh):
    spec = P("outer", None, "inner")
    return jax.shard_map(
        functools.partial(per_device, mesh.shape["inner"]),
        mesh=mesh,
        in_specs=(spec, spec, spec),
        out_specs=P(("outer", "inner"), None, None),
        check_vma=False,
    )
```

```python
import functools
import math

import jax
import jax.numpy as jnp
from jax import lax
from jax.experimental import pallas as pl
from jax.experimental.pallas import tpu as pltpu
from jax.sharding import PartitionSpec as P

HEAD_DIM = 128
XS = 4
ZS = 4
CUTS = 4
FACTOR = math.log2(math.e) / math.sqrt(HEAD_DIM)
MESH = pl.DeviceIdType.MESH


def kernel(
    ni, tok, q_hbm, k_hbm, v_hbm, out_ref,
    raw, qd, kvd, qb, kvb, acc, peak, ob, obuf,
    score_a, score_b, peak_a, peak_b, shrink_a, shrink_b,
    load, zsend, zrecv, xsend, xrecv, osend, orecv,
):
    piece = tok // CUTS
    rows_to = tok // ni
    outer, inner = lax.axis_index("outer"), lax.axis_index("inner")
    x, zl = outer % XS, outer // XS
    core, group = inner % 2, inner // 2
    z_hi, y = group % 2, group // 2
    right, left, far = (x + 1) % XS, (x + XS - 1) % XS, (x + 2) % XS

    def at(x_at, z_at, inner_at):
        return {"outer": z_at * XS + x_at, "inner": inner_at}

    loads = [pltpu.make_async_copy(ref, raw.at[i], load.at[i]) for i, ref in enumerate((q_hbm, k_hbm, v_hbm))]
    for copy in loads:
        copy.start()

    barrier = pltpu.get_barrier_semaphore()

    def hello(index, carry):
        z_at, inner_at = index // ni, index % ni

        @pl.when(jnp.logical_or(z_at != zl, inner_at != inner))
        def _():
            pl.semaphore_signal(barrier, inc=1, device_id=at(x, z_at, inner_at), device_id_type=MESH)

        return carry

    lax.fori_loop(0, ZS * ni, hello, 0)
    for x_at in (left, right):
        pl.semaphore_signal(barrier, inc=1, device_id=at(x_at, zl, inner), device_id_type=MESH)

    acc[...] = jnp.zeros_like(acc)
    peak[...] = jnp.full_like(peak, -1e30)

    span = min(128, piece)
    row = lax.broadcasted_iota(jnp.int32, (2 * span, 2 * span), 0)
    col = lax.broadcasted_iota(jnp.int32, (2 * span, 2 * span), 1)
    take = jnp.where(row < span, 2 * row, 2 * (row - span) + 1)
    sort = jnp.where(col == take, 1.0, 0.0).astype(jnp.bfloat16)
    for i in range(3):
        loads[i].wait()
        for s in range(tok // span):
            mixed = raw[i, s * span:(s + 1) * span].reshape(2 * span, 2 * HEAD_DIM)
            parted = jnp.dot(sort, mixed, preferred_element_type=jnp.float32).astype(jnp.bfloat16)
            for net in range(2):
                for hh in range(2):
                    part = parted[net * span:(net + 1) * span, hh * HEAD_DIM:(hh + 1) * HEAD_DIM]
                    if i == 0:
                        qd[net, hh, s * span:(s + 1) * span] = part
                    else:
                        r, off = s * span // piece, s * span % piece
                        kvd[net, hh, r, i - 1, off:off + span] = part

    keeps = zl // 2 == core
    mine, side = zl % 2, zl // 2

    @pl.when(keeps)
    def _():
        qb[zl] = qd[core, mine]
        for r in range(CUTS):
            kvb[zl, r, x] = kvd[core, mine, r]

    pl.semaphore_wait(barrier, ZS * ni - 1 + 2)

    def z_copy(what, hh, net):
        if what == 0:
            src, dst = qd.at[net, hh], qb.at[zl]
        else:
            src, dst = kvd.at[net, hh, what - 1], kvb.at[zl, what - 1, x]
        return pltpu.make_async_remote_copy(
            src_ref=src, dst_ref=dst,
            send_sem=zsend.at[what, hh, net], recv_sem=zrecv.at[what, zl],
            device_id=at(x, 2 * core + hh, group * 2 + net), device_id_type=MESH,
        )

    def to_all(act, order):
        for what in order:
            for hh in range(2):
                for net in range(2):
                    goes = jnp.logical_or(2 * core + hh != zl, net != core)

                    @pl.when(goes)
                    def _(what=what, hh=hh, net=net):
                        act(z_copy(what, hh, net))

    across = jnp.logical_not(keeps)
    at_end = jnp.logical_or(zl == 0, zl == ZS - 1)

    def start(cond, order):
        pl.when(cond)(lambda: to_all(lambda copy: copy.start(), order))

    start(keeps, (1, 2, 0, 3, 4))
    start(jnp.logical_and(across, at_end), (0, 1, 2, 3, 4))
    start(jnp.logical_and(across, jnp.logical_not(at_end)), (1, 2, 3, 4, 0))

    z_of = (zl, zl + 1 - 2 * mine, (ZS - 1) * (1 - side), 2 - side)

    def wait_for(ref, sem):
        pltpu.make_async_remote_copy(
            src_ref=ref, dst_ref=ref, send_sem=sem, recv_sem=sem,
            device_id=at(right, zl, inner), device_id_type=MESH,
        ).wait_recv()

    def z_arrived(what, j):
        z_at = z_of[j]
        ref = qb.at[z_at] if what == 0 else kvb.at[z_at, what - 1, x]
        if j == 0:
            @pl.when(jnp.logical_not(keeps))
            def _():
                wait_for(ref, zrecv.at[what, z_at])
        else:
            wait_for(ref, zrecv.at[what, z_at])

    def x_copy(kind, j, r):
        block = kvb.at[z_of[j], r]
        ref = (block.at[x], block.at[x], block.at[left, 0], block.at[right, 1])[kind]
        return pltpu.make_async_remote_copy(
            src_ref=ref, dst_ref=ref,
            send_sem=xsend.at[kind, j, r], recv_sem=xrecv.at[kind, j, r],
            device_id=at((right, left)[kind % 2], zl, inner), device_id_type=MESH,
        )

    def x_arrived(kind, j, r):
        block = kvb.at[z_of[j], r]
        ref = (block.at[left], block.at[right], block.at[far, 0], block.at[far, 1])[kind]
        wait_for(ref, xrecv.at[kind, j, r])

    def stage_a(j, r):
        z_arrived(1 + r, j)
        x_copy(0, j, r).start()
        x_copy(1, j, r).start()

    def stage_b(j, r):
        x_arrived(0, j, r)
        x_copy(2, j, r).start()
        x_arrived(1, j, r)
        x_copy(3, j, r).start()

    def stage_c(j, r):
        x_arrived(2, j, r)
        x_arrived(3, j, r)

    width = 2 * XS * piece
    buffers = ((score_a, peak_a, shrink_a), (score_b, peak_b, shrink_b))

    def order(b):
        return z_of[b]

    def rows_of(b):
        return pl.ds(pl.multiple_of(order(b) * tok, tok), tok)

    def scores(z_at, first, b, into):
        score, top, shrink = buffers[into % 2]
        keys = kvb[z_at, pl.ds(first, 2), :, 0].reshape(width, HEAD_DIM)
        s = lax.dot_general(qb[order(b)], keys, (((1,), (1,)), ((), ())), preferred_element_type=jnp.float32)
        score[...] = s
        before = peak[rows_of(b)]
        now = jnp.maximum(before, jnp.max(s, axis=1, keepdims=True) * FACTOR)
        peak[rows_of(b)] = now
        top[...] = now
        shrink[...] = jnp.exp2(before - now)

    def apply(z_at, first, b, into):
        score, top, shrink = buffers[into % 2]
        weights = jnp.exp2(score[...] * FACTOR - jnp.tile(top[...], (1, width // HEAD_DIM)))
        values = kvb[z_at, pl.ds(first, 2), :, 1].reshape(width, HEAD_DIM)
        wide = jnp.concatenate([values, jnp.ones_like(values)], axis=1)
        new = jnp.dot(weights.astype(jnp.bfloat16), wide, preferred_element_type=jnp.float32)
        return acc[rows_of(b)] * jnp.tile(shrink[...], (1, 2)) + new

    def fold(*keys):
        scores(*keys, 0, 0)
        for b in range(ZS - 1):
            if b + 2 < ZS:
                scores(*keys, b + 1, b + 1)
            acc[rows_of(b)] = apply(*keys, b, b)

    slot = core * 2 * ni + group * 4 + zl

    def o_send(b):
        z_at = order(b)
        for e in range(ni):
            z_hi_at = (1 - z_hi if e < ni // 2 else z_hi) if ni > 2 else z_hi
            y_at = (y + 1 + (e % (ni // 2)) // 2) % (ni // 4) if ni > 2 else y
            inner_at = (y_at * 2 + z_hi_at) * 2 + (core + 1 + e) % 2
            if b == 0 and e == ni - 1:
                continue
            pltpu.make_async_remote_copy(
                src_ref=ob.at[z_at * ni + inner_at], dst_ref=obuf.at[slot], send_sem=osend, recv_sem=orecv,
                device_id=at(x, z_at, inner_at), device_id_type=MESH,
            ).start()

    def finish(b, total):
        done = (total[:, :HEAD_DIM] / total[:, HEAD_DIM:]).astype(jnp.bfloat16)
        ob[pl.ds(order(b) * ni, ni)] = done.reshape(ni, rows_to, HEAD_DIM)
        o_send(b)

    A, B, C = stage_a, stage_b, stage_c
    for r in range(CUTS):
        A(0, r)
    B(0, 0), A(1, 0), B(0, 1), A(3, 0), B(0, 2), A(1, 1), B(0, 3), B(1, 0)
    for j in range(ZS - 1):
        z_arrived(0, j)

    chunks = ((0, 0), (0, 2), (1, 0), (3, 0), (1, 2), (2, 0), (2, 2), (3, 2))
    def of(step):
        return z_of[chunks[step][0]], chunks[step][1]

    plan = (
        ((C, 0, 0), (C, 0, 1)),
        ((B, 3, 0), (A, 3, 1), (B, 1, 1), (C, 0, 2), (C, 0, 3)),
        ((A, 1, 2), (B, 3, 1), (A, 2, 0), (A, 3, 2), (C, 1, 0), (C, 1, 1)),
        ((A, 1, 3), (A, 2, 1), (B, 1, 2), (B, 3, 2), (B, 2, 0), (A, 2, 2), (C, 3, 0), (C, 3, 1)),
        ((B, 1, 3), (A, 2, 3), (B, 2, 1), (C, 1, 2), (A, 3, 3), (C, 1, 3)),
        ((B, 2, 2), (C, 2, 0), (C, 2, 1), (B, 2, 3)),
        ((B, 3, 3), (C, 2, 2), (C, 2, 3)),
    )
    for step in range(7):
        for act, j, r in plan[step]:
            act(j, r)
        fold(*of(step))

    late = ZS - 1


    def catch_up(begin, end):
        scores(*of(begin), late, begin)
        for step in range(begin, end):
            if step + 1 < end:
                scores(*of(step + 1), late, step + 1)
            total = apply(*of(step), late, step)
            if step == 7:
                finish(late, total)
            else:
                acc[rows_of(late)] = total

    C(3, 2), C(3, 3)
    scores(*of(7), 0, 0)
    for b in range(ZS - 1):
        if b + 2 < ZS:
            scores(*of(7), b + 1, b + 1)
        finish(b, apply(*of(7), b, b))
    z_arrived(0, 3)
    catch_up(0, 8)
    obuf[slot] = ob[zl * ni + inner]

    to_all(lambda copy: copy.wait_send(), range(1 + CUTS))
    for kind in range(4):
        for j in range(ZS):
            for r in range(CUTS):
                x_copy(kind, j, r).wait_send()
    rest = pltpu.make_async_remote_copy(
        src_ref=obuf.at[pl.ds(0, ZS * ni - 1)], dst_ref=obuf.at[pl.ds(0, ZS * ni - 1)],
        send_sem=osend, recv_sem=orecv, device_id=at(right, zl, inner), device_id_type=MESH,
    )
    rest.wait_send()
    rest.wait_recv()
    out_ref[...] = obuf[...]


def per_device(ni, queries, keys, values):
    tok, nets, cols = queries.shape
    heads = 2 * ni
    rows_to = tok // ni
    piece = tok // CUTS
    hbm = pl.BlockSpec(memory_space=pltpu.HBM)
    dma = pltpu.SemaphoreType.DMA
    bf16, f32 = jnp.bfloat16, jnp.float32
    out = pl.pallas_call(
        functools.partial(kernel, ni, tok),
        out_shape=jax.ShapeDtypeStruct((nets * heads, rows_to, HEAD_DIM), bf16),
        in_specs=[hbm] * 3,
        out_specs=pl.BlockSpec(memory_space=pltpu.VMEM),
        scratch_shapes=[
            pltpu.VMEM((3, tok, nets, cols), bf16),
            pltpu.VMEM((nets, 2, tok, HEAD_DIM), bf16),
            pltpu.VMEM((nets, 2, CUTS, 2, piece, HEAD_DIM), bf16),
            pltpu.VMEM((ZS, tok, HEAD_DIM), bf16),
            pltpu.VMEM((ZS, CUTS, XS, 2, piece, HEAD_DIM), bf16),
            pltpu.VMEM((ZS * tok, 2 * HEAD_DIM), f32),
            pltpu.VMEM((ZS * tok, HEAD_DIM), f32),
            pltpu.VMEM((ZS * ni, rows_to, HEAD_DIM), bf16),
            pltpu.VMEM((nets * heads, rows_to, HEAD_DIM), bf16),
            pltpu.VMEM((tok, 2 * XS * piece), f32),
            pltpu.VMEM((tok, 2 * XS * piece), f32),
            pltpu.VMEM((tok, HEAD_DIM), f32),
            pltpu.VMEM((tok, HEAD_DIM), f32),
            pltpu.VMEM((tok, HEAD_DIM), f32),
            pltpu.VMEM((tok, HEAD_DIM), f32),
            dma((3,)),
            dma((1 + CUTS, 2, 2)),
            dma((1 + CUTS, ZS)),
            dma((4, ZS, CUTS)),
            dma((4, ZS, CUTS)),
            dma,
            dma,
        ],
        compiler_params=pltpu.CompilerParams(collective_id=0, has_side_effects=True, vmem_limit_bytes=53 << 20),
        name="attend",
    )(queries, keys, values)
    return out.reshape(nets, heads, rows_to, HEAD_DIM).transpose(2, 0, 1, 3).reshape(rows_to, nets, heads * HEAD_DIM)


def solution(mesh):
    spec = P("outer", None, "inner")
    return jax.shard_map(
        functools.partial(per_device, mesh.shape["inner"]),
        mesh=mesh,
        in_specs=(spec, spec, spec),
        out_specs=P(("outer", "inner"), None, None),
        check_vma=False,
    )
```
